512 devices in a mesh: lat: 128 (over y, z, core), tok: 4 (over x).
Axes of the slice: x: 4, y: 4, z: 16, core: 2. Of those that a mesh axis runs over, the one named last changes fastest.
Arguments:
- inputs: bfloat16 [256, 3, 2304], P('lat', None, 'tok'), may hold values from -6 to 6
- targets: bfloat16 [256, 3, 2304], P('lat', None, 'tok'), may hold values from -6 to 6
- enc_weight: bfloat16 [3, 2304, 32768], P(None, 'tok', 'lat'), may hold values from -0.125 to 0.125
- enc_bias: float32 [3, 32768], P(None, 'lat'), may hold values from -3 to 3
- dec_weight: bfloat16 [6, 32768, 2304], P(None, 'lat', 'tok'), may hold values from -0.03125 to 0.03125
- counts: int32 [3, 128], P(None, 'lat'), may hold values from 32 to 256, as said below
Outputs:
- recon: bfloat16 [256, 3, 2304], P('lat', None, 'tok')
- dec_grad: bfloat16 [6, 32768, 2304], P(None, 'lat', 'tok')
- latent_grad: bfloat16 [256, 3, 32768], P('tok', None, 'lat')
The draws below stay inside these ranges and needn't reach their ends.
Inputs may be any that keep to these rules, and one draw needn't show every extreme that they name: Latents 0 to counts[l, t] - 1 of layer l's tile on index t of lat are live, the rest dead; in every layer some tile has all 256 live.
All inputs are finite; a program needn't handle non-finite values.
Results may differ from the reference program's by a relative error of at most 0.0054.
Values may be sent and summed in bfloat16 or wider, within the bound.
A program may use at most 64 MiB of HBM per device.

```python
import jax
import jax.numpy as jnp

D = 2304
LAT_DEV = 256
L = 3
TOKENS = 256
LATENTS = 32768
BLOCKS = 6
N_LAT = 128


def draw_counts(key, part):
    first_key, second_key = jax.random.split(key, 2)
    spread = 7 * LAT_DEV // 8
    raw_values = jax.random.randint(first_key, (L, N_LAT), 0, spread + 1)
    skewed = LAT_DEV // 8 + raw_values * raw_values // spread
    full_tile = jax.random.randint(second_key, (L,), 0, N_LAT)
    chosen = jnp.arange(N_LAT, dtype=jnp.int32)[None, :] == full_tile[:, None]
    return jnp.where(chosen, LAT_DEV, skewed).astype(jnp.int32)


def steps_of(key, shape, cuts, smallest, largest):
    def one(axis_at, blocks):
        steps = jax.random.uniform(jax.random.fold_in(jax.random.fold_in(key, 6), axis_at), (blocks,), jnp.float32, smallest / len(cuts), largest / len(cuts))
        return jnp.repeat(jnp.exp(steps), shape[axis_at] // blocks).reshape((-1,) + (1,) * (len(shape) - axis_at - 1))

    factor_of = one(*cuts[0])
    for cut in cuts[1:]:
        factor_of = factor_of * one(*cut)
    return factor_of


def centred(key, shape, deviation, most, cuts=(), held_as=jnp.bfloat16):
    gain = steps_of(key, shape, cuts, -0.22, 0.18) if cuts else 1.0
    entries = jax.random.normal(key, shape, jnp.float32) * deviation * gain
    return jnp.minimum(jnp.maximum(entries, -most), most).astype(held_as)


def setup_inputs(seed: int = 0) -> dict:
    key_list = jax.random.split(jax.random.key(seed), 7)
    inputs = centred(key_list[0], (TOKENS, L, D), 1.0, 6.0, ((0, 128), (2, 4)))
    targets = centred(key_list[1], (TOKENS, L, D), 1.0, 6.0, ((0, 128), (2, 4)))
    enc_weight = centred(key_list[2], (L, D, LATENTS), D ** -0.5, 0.125, ((1, 4), (2, 128)))
    enc_bias = centred(key_list[3], (L, LATENTS), 0.5, 3.0, ((1, 128),), jnp.float32)
    dec_weight = centred(key_list[4], (BLOCKS, LATENTS, D), (LAT_DEV * N_LAT) ** -0.5, 0.03125, ((1, 128), (2, 4)))
    counts = draw_counts(jax.random.fold_in(key_list[6], 71), 0)
    return dict(inputs=inputs, targets=targets, enc_weight=enc_weight, enc_bias=enc_bias, dec_weight=dec_weight, counts=counts)


def block_index(source, target):
    return source * L - source * (source - 1) // 2 + (target - source)


def reference(inputs, targets, enc_weight, enc_bias, dec_weight, counts):
    positions = jnp.arange(LAT_DEV * N_LAT, dtype=jnp.int32)
    live_mask = (positions % LAT_DEV)[None, :] < jnp.repeat(counts, LAT_DEV, axis=1)
    latents = []
    for source in range(L):
        preact = jnp.dot(inputs[:, source, :], enc_weight[source], preferred_element_type=jnp.float32)
        preact = preact + enc_bias[source][None, :]
        latents.append(jnp.where(live_mask[source][None, :], jnp.maximum(preact, 0.0), 0.0).astype(jnp.bfloat16))
    recons = []
    errors = []
    for target in range(L):
        summed = jnp.zeros((TOKENS, D), jnp.float32)
        for source in range(target + 1):
            summed = summed + jnp.dot(latents[source], dec_weight[block_index(source, target)], preferred_element_type=jnp.float32)
        recons.append(summed.astype(jnp.bfloat16))
        errors.append((summed - targets[:, target, :].astype(jnp.float32)).astype(jnp.bfloat16))
    grads = []
    for source in range(L):
        for target in range(source, L):
            grads.append(jnp.dot(latents[source].T, errors[target], preferred_element_type=jnp.float32).astype(jnp.bfloat16))
    latent_grads = []
    for source in range(L):
        summed = jnp.zeros((TOKENS, LAT_DEV * N_LAT), jnp.float32)
        for target in range(source, L):
            summed = summed + jnp.dot(errors[target], dec_weight[block_index(source, target)].T, preferred_element_type=jnp.float32)
        latent_grads.append(jnp.where(live_mask[source][None, :], summed, 0.0).astype(jnp.bfloat16))
    return jnp.stack(recons, axis=1), jnp.stack(grads, axis=0), jnp.stack(latent_grads, axis=1)
```

```python
import functools

import jax
import jax.numpy as jnp
from jax import lax
from jax.experimental import pallas as pl
from jax.experimental.pallas import tpu as pltpu
from jax.sharding import PartitionSpec as P

MESH = pl.DeviceIdType.MESH
F32 = jnp.float32
BF16 = jnp.bfloat16

STEPS = {
    "a1": 9.0, "a2": 13.0, "a3": 15.0, "b1": 19.0, "b2": 23.0, "c1": 25.0,
    "c2": 29.0, "c3": 38.0, "d1": 47.0, "d2": 51.0, "d3": 53.0,
}
SPACING = 1.8


def block_index(source, target, layers):
    return source * layers - source * (source - 1) // 2 + (target - source)


def dot_nn(a, b):
    return lax.dot_general(a, b, (((1,), (0,)), ((), ())), preferred_element_type=F32)


def dot_nt(a, b):
    return lax.dot_general(a, b, (((1,), (1,)), ((), ())), preferred_element_type=F32)


def dot_tn(a, b):
    return lax.dot_general(a, b, (((0,), (0,)), ((), ())), preferred_element_type=F32)


def kernel(
    sizes,
    in_hbm, tg_hbm, ew_hbm, bias_hbm, dw_hbm, cnt_hbm,
    recon_ref, dg_ref, lg_ref,
    own_in, tg, ew, bias, cnt, dw,
    zin, ga, pf, pp, pr, lt, rf, cr, ys, yr, zf, zs, zr, own_er, ez, ge, ef, es, er,
    load_sem, z_send, z_recv, y_send, y_recv, x_send, x_recv, c_send, c_recv,
):
    ny, nz, nx = sizes
    layers, pair, width = own_in.shape
    tile = ew.shape[2]
    rows = nz * pair
    tokens = 2 * ny * rows
    lat = lax.axis_index("lat")
    x = lax.axis_index("tok")
    c = lax.rem(lat, 2)
    z = lax.rem(lax.div(lat, 2), nz)
    y = lax.div(lat, 2 * nz)
    mate = 1 - c

    def device(y_at, z_at, c_at, x_at):
        return {"lat": (y_at * nz + z_at) * 2 + c_at, "tok": x_at}

    def z_peer(k):
        return device(y, k, c, x)

    def y_peer(k):
        return device(k, z, c, x)

    def x_peer(k):
        return device(y, z, c, k)

    loads = [
        pltpu.make_async_copy(src, dst, load_sem.at[i])
        for i, (src, dst) in enumerate(
            ((in_hbm, own_in), (tg_hbm, tg), (bias_hbm, bias), (cnt_hbm, cnt), (ew_hbm, ew), (dw_hbm, dw))
        )
    ]
    for load in loads:
        load.start()

    barrier = pltpu.get_barrier_semaphore()

    def greet(count, me, peer):
        @pl.loop(1, count)
        def _(k):
            pl.semaphore_signal(
                barrier, inc=1, device_id=peer(lax.rem(me + k, count)), device_id_type=MESH
            )

    greet(nz, z, z_peer)
    greet(ny, y, y_peer)
    greet(nx, x, x_peer)
    pl.semaphore_signal(barrier, inc=1, device_id=device(y, z, mate, x), device_id_type=MESH)
    pl.semaphore_wait(barrier, nz + ny + nx - 2)

    def remote(src, dst, send, recv, to):
        return pltpu.make_async_remote_copy(
            src_ref=src, dst_ref=dst, send_sem=send, recv_sem=recv, device_id=to, device_id_type=MESH
        )

    def exchange(phase, l, count, me, peer, send, recv, part, slot):
        half = count // 2

        def start():
            @pl.loop(0, count - 1)
            def _(k):
                far = half - lax.div(k + 1, 2)
                sign = 1 - 2 * lax.rem(k + 1, 2)
                to = lax.rem(me + count + sign * far, count)
                remote(part(to), slot(me), send.at[phase, l, to], recv.at[phase, l, me], peer(to)).start()

        def arrive():
            @pl.loop(1, count)
            def _(k):
                k = lax.rem(me + k, count)
                remote(part(k), slot(k), send.at[phase, l, k], recv.at[phase, l, k], peer(k)).wait_recv()

        def drain():
            @pl.loop(1, count)
            def _(k):
                k = lax.rem(me + k, count)
                remote(part(k), slot(k), send.at[phase, l, k], recv.at[phase, l, k], peer(k)).wait_send()

        return start, arrive, drain

    def z_exchange(phase, l, part, slot):
        return exchange(phase, l, nz, z, z_peer, z_send, z_recv, part, slot)

    def y_exchange(phase, l, part, slot):
        return exchange(phase, l, ny, y, y_peer, y_send, y_recv, part, slot)

    def x_exchange(phase, l, part, slot):
        return exchange(phase, l, nx, x, x_peer, x_send, x_recv, part, slot)

    def swap(phase, l, src, dst):
        return remote(src, dst, c_send.at[phase, l], c_recv.at[phase, l], device(y, z, mate, x))

    every = range(layers)
    a1 = [z_exchange(0, l, lambda k, l=l: own_in.at[l], lambda k, l=l: zin.at[l, k]) for l in every]
    c3 = [z_exchange(1, l, lambda k, l=l: zs.at[l, k], lambda k, l=l: zr.at[l, k]) for l in every]
    d1 = [z_exchange(2, l, lambda k, l=l: own_er.at[l], lambda k, l=l: ez.at[l, k]) for l in every]
    a2 = [y_exchange(0, l, lambda k, l=l: ga.at[l, c, y], lambda k, l=l: ga.at[l, c, k]) for l in every]
    c2 = [y_exchange(1, l, lambda k, l=l: ys.at[l, k], lambda k, l=l: yr.at[l, k]) for l in every]
    d2 = [y_exchange(2, l, lambda k, l=l: ge.at[l, c, y], lambda k, l=l: ge.at[l, c, k]) for l in every]
    b1 = [x_exchange(0, l, lambda k, l=l: pp.at[l, :, k], lambda k, l=l: pr.at[l, k]) for l in every]
    b2 = [x_exchange(1, l, lambda k, l=l: lt.at[l, :, x], lambda k, l=l: lt.at[l, :, k]) for l in every]
    e1 = [x_exchange(2, l, lambda k, l=l: es.at[l, :, k], lambda k, l=l: er.at[l, k]) for l in every]
    a3 = [swap(0, l, ga.at[l, c], ga.at[l, c]) for l in every]
    a3_in = [swap(0, l, ga.at[l, mate], ga.at[l, mate]) for l in every]
    c1 = [swap(1, l, rf.at[l, mate], cr.at[l]) for l in every]
    d3 = [swap(2, l, ge.at[l, c], ge.at[l, c]) for l in every]
    d3_in = [swap(2, l, ge.at[l, mate], ge.at[l, mate]) for l in every]

    loads[0].wait()
    for l in every:
        a1[l][0]()
    for l in every:
        zin[l, z] = own_in[l]
    for load in loads[1:]:
        load.wait()

    def live(l):
        return lax.broadcasted_iota(jnp.int32, (1, tile), 1) < cnt[0:1, l : l + 1]

    def joined(blocks):
        return blocks.astype(F32).reshape(rows, width).astype(BF16)

    def step_a1(l):
        a1[l][1]()
        ga[l, c, y] = joined(zin[l])
        a2[l][0]()

    def step_a2(l):
        a2[l][1]()
        a3[l].start()

    def step_a3(l):
        a3_in[l].wait_recv()
        partial = dot_nn(ga[l].reshape(tokens, width), ew[l]).reshape(2, ny, rows, tile)
        pf[l] = partial
        pp[l] = partial.astype(BF16)
        b1[l][0]()

    def step_b1(l):
        b1[l][1]()
        summed = pf[l, :, x]
        for k in range(1, nx):
            summed = summed + pr[l, lax.rem(x + k, nx)].astype(F32)
        summed = summed + bias[l : l + 1, :].reshape(1, 1, tile)
        alive = live(l).reshape(1, 1, tile)
        lt[l, :, x] = jnp.where(alive, jnp.maximum(summed, 0.0), 0.0).astype(BF16)
        b2[l][0]()

    def step_b2(m):
        b2[m][1]()
        total = None
        for l in range(m + 1):
            term = dot_nt(lt[l].reshape(tokens, tile), dw[block_index(l, m, layers)])
            total = term if total is None else total + term
        rf[m] = total.reshape(2, ny, rows, width)
        c1[m].start()

    def step_c1(m):
        c1[m].wait_recv()
        ys[m] = (rf[m, c] + cr[m]).astype(BF16)
        c2[m][0]()

    def step_c2(m):
        c2[m][1]()
        summed = rf[m, c, y] + cr[m, y]
        for k in range(1, ny):
            summed = summed + yr[m, lax.rem(y + k, ny)].astype(F32)
        blocks = summed.reshape(nz, pair, width)
        zf[m] = blocks
        zs[m] = blocks.astype(BF16)
        c3[m][0]()

    def step_c3(m):
        c3[m][1]()
        full = zf[m, z]
        for k in range(1, nz):
            full = full + zr[m, lax.rem(z + k, nz)].astype(F32)
        errors = (full - tg[m].astype(F32)).astype(BF16)
        own_er[m] = errors
        d1[m][0]()
        ez[m, z] = errors
        recon_ref[m] = full.astype(BF16)

    def step_d1(m):
        d1[m][1]()
        ge[m, c, y] = joined(ez[m])
        d2[m][0]()

    def step_d2(m):
        d2[m][1]()
        d3[m].start()

    def step_d3(m):
        d3_in[m].wait_recv()
        rows_of = ge[m].reshape(tokens, width)
        for l in range(m + 1):
            term = dot_nn(rows_of, dw[block_index(l, m, layers)]).reshape(2, ny, rows, tile)
            term = term if l == m else ef[l] + term
            ef[l] = term
            if m == layers - 1:
                es[l] = term.astype(BF16)
                e1[l][0]()
        for l in range(m + 1):
            dg_ref[block_index(l, m, layers)] = dot_tn(rows_of, lt[l].reshape(tokens, tile)).astype(BF16)

    acts = dict(
        a1=step_a1, a2=step_a2, a3=step_a3, b1=step_b1, b2=step_b2, c1=step_c1,
        c2=step_c2, c3=step_c3, d1=step_d1, d2=step_d2, d3=step_d3,
    )
    order = sorted((at + SPACING * l, name, l) for name, at in STEPS.items() for l in every)
    for _, name, l in order:
        acts[name](l)

    for l in every:
        e1[l][1]()
        summed = ef[l, :, x]
        for k in range(1, nx):
            summed = summed + er[l, lax.rem(x + k, nx)].astype(F32)
        lg_ref[l] = jnp.where(live(l).reshape(1, 1, tile), summed, 0.0).astype(BF16)

    for group in (a1, a2, b1, b2, c2, c3, d1, d2, e1):
        for l in every:
            group[l][2]()
    for group in (a3, c1, d3):
        for l in every:
            group[l].wait_send()


def build(mesh, sizes):
    ny, nz, nx = sizes

    def local(inputs, targets, enc_weight, enc_bias, dec_weight, counts):
        pair, layers, width = inputs.shape
        tile = enc_weight.shape[2]
        blocks = dec_weight.shape[0]
        rows = nz * pair
        in_hbm = pl.BlockSpec(memory_space=pltpu.HBM)
        in_vmem = pl.BlockSpec(memory_space=pltpu.VMEM)

        def vmem(*shape, dtype=BF16):
            return pltpu.VMEM(shape, dtype)

        def sems(*shape):
            return pltpu.SemaphoreType.DMA(shape)

        recon, dec_grad, latent_grad = pl.pallas_call(
            functools.partial(kernel, sizes),
            out_shape=(
                jax.ShapeDtypeStruct((layers, pair, width), BF16),
                jax.ShapeDtypeStruct((blocks, width, tile), BF16),
                jax.ShapeDtypeStruct((layers, 2, rows, tile), BF16),
            ),
            in_specs=[in_hbm] * 6,
            out_specs=(in_vmem, in_vmem, in_vmem),
            scratch_shapes=[
                vmem(layers, pair, width),
                vmem(layers, pair, width),
                vmem(layers, width, tile),
                vmem(layers, tile, dtype=F32),
                vmem(1, layers, dtype=jnp.int32),
                vmem(blocks, width, tile),
                vmem(layers, nz, pair, width),
                vmem(layers, 2, ny, rows, width),
                vmem(layers, 2, ny, rows, tile, dtype=F32),
                vmem(layers, 2, ny, rows, tile),
                vmem(layers, nx, 2, rows, tile),
                vmem(layers, 2, ny, rows, tile),
                vmem(layers, 2, ny, rows, width, dtype=F32),
                vmem(layers, ny, rows, width, dtype=F32),
                vmem(layers, ny, rows, width),
                vmem(layers, ny, rows, width),
                vmem(layers, nz, pair, width, dtype=F32),
                vmem(layers, nz, pair, width),
                vmem(layers, nz, pair, width),
                vmem(layers, pair, width),
                vmem(layers, nz, pair, width),
                vmem(layers, 2, ny, rows, width),
                vmem(layers, 2, ny, rows, tile, dtype=F32),
                vmem(layers, 2, ny, rows, tile),
                vmem(layers, nx, 2, rows, tile),
                sems(6),
                sems(3, layers, nz), sems(3, layers, nz),
                sems(3, layers, ny), sems(3, layers, ny),
                sems(3, layers, nx), sems(3, layers, nx),
                sems(3, layers), sems(3, layers),
            ],
            compiler_params=pltpu.CompilerParams(
                collective_id=0, has_side_effects=True, vmem_limit_bytes=48 * 1024 * 1024
            ),
        )(
            inputs.transpose(1, 0, 2),
            targets.transpose(1, 0, 2),
            enc_weight,
            enc_bias,
            dec_weight.transpose(0, 2, 1),
            counts.T,
        )
        latent_grad = latent_grad.reshape(layers, 2, nz, pair, tile).transpose(2, 1, 3, 0, 4)
        return (
            recon.transpose(1, 0, 2),
            dec_grad.transpose(0, 2, 1),
            latent_grad.reshape(2 * rows, layers, tile),
        )

    in_specs = (
        P("lat", None, "tok"),
        P("lat", None, "tok"),
        P(None, "tok", "lat"),
        P(None, "lat"),
        P(None, "lat", "tok"),
        P(None, "lat"),
    )
    out_specs = (P("lat", None, "tok"), P(None, "lat", "tok"), P("tok", None, "lat"))
    return jax.shard_map(local, mesh=mesh, in_specs=in_specs, out_specs=out_specs, check_vma=False)


def solution(mesh):
    nx = mesh.shape["tok"]
    return build(mesh, (4, mesh.shape["lat"] // 8, nx))
```

```python
import functools

import jax
import jax.numpy as jnp
from jax import lax
from jax.experimental import pallas as pl
from jax.experimental.pallas import tpu as pltpu
from jax.sharding import PartitionSpec as P

MESH = pl.DeviceIdType.MESH
F32 = jnp.float32
BF16 = jnp.bfloat16

CLASSES = 2

STEPS = {
    "a1": 15.0, "a2": 18.5, "a3": 19.5, "b1": 23.0, "b2": 26.0, "c1": 28.0,
    "c2": 31.5, "c3": 38.0, "d1": 43.5, "d2": 47.5, "d3": 48.5,
}
SPACING = 0.85


def block_index(source, target, layers):
    return source * layers - source * (source - 1) // 2 + (target - source)


def dot_nn(a, b):
    return lax.dot_general(a, b, (((1,), (0,)), ((), ())), preferred_element_type=F32)


def dot_nt(a, b):
    return lax.dot_general(a, b, (((1,), (1,)), ((), ())), preferred_element_type=F32)


def dot_tn(a, b):
    return lax.dot_general(a, b, (((0,), (0,)), ((), ())), preferred_element_type=F32)


def far_first(count):
    return sorted(range(1, count), key=lambda k: -min(k, count - k))


def kernel(
    sizes,
    in_hbm, tg_hbm, ew_hbm, bias_hbm, dw_hbm, cnt_hbm,
    recon_ref, dg_ref, lg_ref,
    own_in, tg, ew, bias, cnt, dw,
    zin, ga, pf, pp, pr, lt, rf, cr, ys, yr, zf, zs, zr, own_er, ez, ge, ef, es, er,
    load_sem, z_send, z_recv, y_send, y_recv, x_send, x_recv, c_send, c_recv,
):
    ny, nz, nx = sizes
    layers, pair, width = own_in.shape
    tile = ew.shape[2]
    classes = zin.shape[1]
    nq = nz // classes
    rows = nq * pair
    half = 2 * ny * rows
    lat = lax.axis_index("lat")
    x = lax.axis_index("tok")
    c = lax.rem(lat, 2)
    z = lax.rem(lax.div(lat, 2), nz)
    y = lax.div(lat, 2 * nz)
    mate = 1 - c
    zh = lax.rem(z, classes)
    zq = lax.div(z, classes)

    def device(y_at, z_at, c_at, x_at):
        return {"lat": (y_at * nz + z_at) * 2 + c_at, "tok": x_at}

    def z_peer(k):
        return device(y, k, c, x)

    def y_peer(k):
        return device(k, z, c, x)

    def x_peer(k):
        return device(y, z, c, k)

    core_peer = device(y, z, mate, x)

    barrier = pltpu.get_barrier_semaphore()
    for count, me, peer in ((nz, z, z_peer), (ny, y, y_peer), (nx, x, x_peer)):
        for k in far_first(count):
            pl.semaphore_signal(
                barrier, inc=1, device_id=peer(lax.rem(me + k, count)), device_id_type=MESH
            )
    pl.semaphore_signal(barrier, inc=1, device_id=core_peer, device_id_type=MESH)

    loads = [
        pltpu.make_async_copy(src, dst, load_sem.at[i])
        for i, (src, dst) in enumerate(
            ((in_hbm, own_in), (tg_hbm, tg), (bias_hbm, bias), (cnt_hbm, cnt), (ew_hbm, ew), (dw_hbm, dw))
        )
    ]
    for load in loads:
        load.start()
    loads[0].wait()
    pl.semaphore_wait(barrier, nz + ny + nx - 2)

    def send(src, dst, send_sem, recv_sem, to):
        pltpu.make_async_remote_copy(
            src_ref=src, dst_ref=dst, send_sem=send_sem, recv_sem=recv_sem, device_id=to, device_id_type=MESH
        ).start()

    def settle(ref, sem):
        pltpu.make_async_copy(ref, ref, sem).wait()

    def span(count):
        return pl.ds(0, count)

    every = range(layers)
    each = range(classes)
    chunks = [(l, h) for l in every for h in each]
    drains = []

    def z_gather(phase, l, h, own, slots):
        sends, recvs = z_send.at[phase, l, h], z_recv.at[phase, l, h]

        def start():
            @pl.when(zh == h)
            def _():
                @pl.loop(0, nz - 1)
                def _(k):
                    far = nz // 2 - lax.div(k + 1, 2)
                    to = lax.rem(z + nz + (1 - 2 * lax.rem(k + 1, 2)) * far, nz)
                    send(own.at[l], slots.at[l, h, zq], sends, recvs, z_peer(to))

        def arrive():
            @pl.when(zh != h)
            def _():
                settle(slots.at[l, h], recvs)

            if nq > 1:
                @pl.when(zh == h)
                def _():
                    settle(slots.at[l, h, span(nq - 1)], recvs)

        def drain():
            @pl.when(zh == h)
            def _():
                settle(zr.at[l, span(nz - 1)], sends)

        drains.append(drain)
        return start, arrive

    def z_scatter(m, h):
        sends, recvs = z_send.at[1, m, h], z_recv.at[1, m, 0]
        shift = lax.rem(h - zh + classes, classes)

        def one(step):
            to = lax.rem(z + shift + classes * step, nz)
            send(zs.at[m, h, lax.div(to, classes)], zr.at[m, z], sends, recvs, z_peer(to))

        def start():
            @pl.loop(0, nq - 1)
            def _(k):
                far = nq // 2 - lax.div(k + 1, 2)
                one(lax.rem(nq + (1 - 2 * lax.rem(k + 1, 2)) * far, nq))

            @pl.when(shift != 0)
            def _():
                one(0)

        def arrive():
            settle(zr.at[m, span(nz - 1)], recvs)

        def drain():
            @pl.when(shift != 0)
            def _():
                settle(zs.at[m, h], sends)

            if nq > 1:
                @pl.when(shift == 0)
                def _():
                    settle(zs.at[m, h, span(nq - 1)], sends)

        drains.append(drain)
        return start, arrive

    def exchange(count, me, peer, sends, recvs, part, slot, landed):
        def start():
            for k in far_first(count):
                to = lax.rem(me + k, count)
                send(part(to), slot(me), sends, recvs, peer(to))

        def arrive():
            settle(landed, recvs)

        def drain():
            settle(landed, sends)

        drains.append(drain)
        return start, arrive

    def y_exchange(phase, l, h, part, slot, landed):
        return exchange(
            ny, y, y_peer, y_send.at[phase, l, h], y_recv.at[phase, l, h], part, slot, landed
        )

    def x_exchange(phase, l, h, part, slot, landed):
        return exchange(
            nx, x, x_peer, x_send.at[phase, l, h], x_recv.at[phase, l, h], part, slot, landed
        )

    def swap(phase, l, h, src, dst, landing):
        sends, recvs = c_send.at[phase, l, h], c_recv.at[phase, l, h]
        drains.append(lambda: settle(landing, sends))
        return (lambda: send(src, dst, sends, recvs, core_peer)), (lambda: settle(landing, recvs))

    def table(make):
        return {(l, h): make(l, h) for l, h in chunks}

    a1 = table(lambda l, h: z_gather(0, l, h, own_in, zin))
    d1 = table(lambda l, h: z_gather(2, l, h, own_er, ez))
    c3 = table(z_scatter)

    def y_gather(phase, held):
        return table(
            lambda l, h: y_exchange(
                phase, l, h, lambda k: held.at[l, h, c, y], lambda k: held.at[l, h, c, k],
                held.at[l, h, c, span(ny - 1)],
            )
        )

    a2, d2 = y_gather(0, ga), y_gather(2, ge)
    c2 = table(
        lambda m, h: y_exchange(
            1, m, h, lambda k: ys.at[m, h, k], lambda k: yr.at[m, h, k], yr.at[m, h, span(ny - 1)]
        )
    )

    def x_scatter(phase, parts, slots):
        return table(
            lambda l, h: x_exchange(
                phase, l, h, lambda k: parts.at[l, h, :, k], lambda k: slots.at[l, h, k],
                slots.at[l, h, span(nx - 1)],
            )
        )

    b1, e1 = x_scatter(0, pp, pr), x_scatter(2, es, er)
    b2 = table(
        lambda l, h: x_exchange(
            1, l, h, lambda k: lt.at[l, h, :, x], lambda k: lt.at[l, h, :, k],
            lt.at[l, h, :, span(nx - 1)],
        )
    )
    a3 = table(lambda l, h: swap(0, l, h, ga.at[l, h, c], ga.at[l, h, c], ga.at[l, h, mate]))
    d3 = table(lambda l, h: swap(2, l, h, ge.at[l, h, c], ge.at[l, h, c], ge.at[l, h, mate]))
    c1 = table(lambda m, h: swap(1, m, h, rf.at[m, h, mate], cr.at[m, h], cr.at[m, h]))

    for chunk in chunks:
        a1[chunk][0]()
    for l in every:
        zin[l, zh, zq] = own_in[l]
    for load in loads[1:]:
        load.wait()

    def live(l):
        return lax.broadcasted_iota(jnp.int32, (1, tile), 1) < cnt[0:1, l : l + 1]

    def joined(blocks):
        return blocks.astype(F32).reshape(rows, width).astype(BF16)

    def step_a1(l, h):
        a1[l, h][1]()
        ga[l, h, c, y] = joined(zin[l, h])
        a2[l, h][0]()

    def step_a2(l, h):
        a2[l, h][1]()
        a3[l, h][0]()

    def step_a3(l, h):
        a3[l, h][1]()
        partial = dot_nn(ga[l, h].reshape(half, width), ew[l]).reshape(2, ny, rows, tile)
        pf[l, h] = partial
        pp[l, h] = partial.astype(BF16)
        b1[l, h][0]()

    def step_b1(l, h):
        b1[l, h][1]()
        summed = pf[l, h, :, x]
        for k in range(1, nx):
            summed = summed + pr[l, h, lax.rem(x + k, nx)].astype(F32)
        summed = summed + bias[l : l + 1, :].reshape(1, 1, tile)
        alive = live(l).reshape(1, 1, tile)
        lt[l, h, :, x] = jnp.where(alive, jnp.maximum(summed, 0.0), 0.0).astype(BF16)
        b2[l, h][0]()

    def step_b2(m, h):
        b2[m, h][1]()
        total = None
        for l in range(m + 1):
            term = dot_nt(lt[l, h].reshape(half, tile), dw[block_index(l, m, layers)])
            total = term if total is None else total + term
        rf[m, h] = total.reshape(2, ny, rows, width)
        c1[m, h][0]()

    def step_c1(m, h):
        c1[m, h][1]()
        ys[m, h] = (rf[m, h, c] + cr[m, h]).astype(BF16)
        c2[m, h][0]()

    def step_c2(m, h):
        c2[m, h][1]()
        summed = rf[m, h, c, y] + cr[m, h, y]
        for k in range(1, ny):
            summed = summed + yr[m, h, lax.rem(y + k, ny)].astype(F32)
        blocks = summed.reshape(nq, pair, width)
        zf[m, h] = blocks
        zs[m, h] = blocks.astype(BF16)
        c3[m, h][0]()

    def step_c3(m, h):
        @pl.when(zh == h)
        def _():
            c3[m, h][1]()
            full = zf[m, h, zq]
            for k in range(1, nz):
                full = full + zr[m, lax.rem(z + k, nz)].astype(F32)
            errors = (full - tg[m].astype(F32)).astype(BF16)
            own_er[m] = errors
            d1[m, h][0]()
            ez[m, h, zq] = errors
            recon_ref[m] = full.astype(BF16)

    def step_d1(m, h):
        d1[m, h][1]()
        ge[m, h, c, y] = joined(ez[m, h])
        d2[m, h][0]()

    def step_d2(m, h):
        d2[m, h][1]()
        d3[m, h][0]()

    def step_d3(m, h):
        d3[m, h][1]()
        rows_of = ge[m, h].reshape(half, width)
        for l in range(m + 1):
            term = dot_nn(rows_of, dw[block_index(l, m, layers)]).reshape(2, ny, rows, tile)
            term = term if l == m else ef[l, h] + term
            ef[l, h] = term
            if m == layers - 1:
                es[l, h] = term.astype(BF16)
                e1[l, h][0]()

    acts = dict(
        a1=step_a1, a2=step_a2, a3=step_a3, b1=step_b1, b2=step_b2, c1=step_c1,
        c2=step_c2, c3=step_c3, d1=step_d1, d2=step_d2, d3=step_d3,
    )
    order = sorted(
        (at + SPACING * i, name, chunk)
        for name, at in STEPS.items()
        for i, chunk in enumerate(chunks)
    )
    for _, name, chunk in order:
        acts[name](*chunk)

    for m in every:
        errors_of = ge[m].reshape(classes * half, width)
        for l in range(m + 1):
            latents_of = lt[l].reshape(classes * half, tile)
            dg_ref[block_index(l, m, layers)] = dot_tn(errors_of, latents_of).astype(BF16)
    late = [(l, h) for h in each for l in every]
    for drain in drains:
        drain()
    for l, h in late:
        e1[l, h][1]()
        summed = ef[l, h, :, x]
        for k in range(1, nx):
            summed = summed + er[l, h, lax.rem(x + k, nx)].astype(F32)
        summed = jnp.where(live(l).reshape(1, 1, tile), summed, 0.0)
        pf[l, h, :, 0] = summed
    for l in every:
        by_owner = pf[l, :, :, 0].reshape(classes, 2, nq, pair, tile).transpose(2, 0, 1, 3, 4)
        lg_ref[l] = by_owner.reshape(classes * 2 * rows, tile).astype(BF16)


def store(a_ref, b_ref, c_ref, a_out, b_out, c_out, sem):
    copies = [
        pltpu.make_async_copy(src, dst, sem.at[i])
        for i, (src, dst) in enumerate(((a_ref, a_out), (b_ref, b_out), (c_ref, c_out)))
    ]
    for copy in copies:
        copy.start()
    for copy in copies:
        copy.wait()


def build(mesh, sizes, classes):
    ny, nz, nx = sizes

    def local(inputs, targets, enc_weight, enc_bias, dec_weight, counts):
        pair, layers, width = inputs.shape
        tile = enc_weight.shape[2]
        blocks = dec_weight.shape[0]
        nq = nz // classes
        rows = nq * pair
        lh = (layers, classes)
        in_hbm = pl.BlockSpec(memory_space=pltpu.HBM)
        in_vmem = pl.BlockSpec(memory_space=pltpu.VMEM)

        def vmem(*shape, dtype=BF16):
            return pltpu.VMEM(shape, dtype)

        def sems(*shape):
            return pltpu.SemaphoreType.DMA(shape)

        operands = (
            inputs.transpose(1, 0, 2),
            targets.transpose(1, 0, 2),
            enc_weight,
            enc_bias,
            dec_weight.transpose(0, 2, 1),
            counts.T,
        )
        computed = pl.pallas_call(
            functools.partial(kernel, sizes),
            out_shape=(
                pltpu.VMEM((layers, pair, width), BF16),
                pltpu.VMEM((blocks, width, tile), BF16),
                pltpu.VMEM((layers, classes * 2 * rows, tile), BF16),
            ),
            in_specs=[in_hbm] * 6,
            out_specs=(in_vmem, in_vmem, in_vmem),
            scratch_shapes=[
                vmem(layers, pair, width),
                vmem(layers, pair, width),
                vmem(layers, width, tile),
                vmem(layers, tile, dtype=F32),
                vmem(1, layers, dtype=jnp.int32),
                vmem(blocks, width, tile),
                vmem(*lh, nq, pair, width),
                vmem(*lh, 2, ny, rows, width),
                vmem(*lh, 2, ny, rows, tile, dtype=F32),
                vmem(*lh, 2, ny, rows, tile),
                vmem(*lh, nx, 2, rows, tile),
                vmem(*lh, 2, ny, rows, tile),
                vmem(*lh, 2, ny, rows, width, dtype=F32),
                vmem(*lh, ny, rows, width, dtype=F32),
                vmem(*lh, ny, rows, width),
                vmem(*lh, ny, rows, width),
                vmem(*lh, nq, pair, width, dtype=F32),
                vmem(*lh, nq, pair, width),
                vmem(layers, nz, pair, width),
                vmem(layers, pair, width),
                vmem(*lh, nq, pair, width),
                vmem(*lh, 2, ny, rows, width),
                vmem(*lh, 2, ny, rows, tile, dtype=F32),
                vmem(*lh, 2, ny, rows, tile),
                vmem(*lh, nx, 2, rows, tile),
                sems(6),
                *(sems(3, *lh) for _ in range(8)),
            ],
            compiler_params=pltpu.CompilerParams(
                collective_id=0, has_side_effects=True, vmem_limit_bytes=48 * 1024 * 1024
            ),
        )(*(pltpu.with_memory_space_constraint(array, pltpu.HBM) for array in operands))
        recon, dec_grad, latent_grad = pl.pallas_call(
            store,
            out_shape=tuple(pltpu.HBM(part.shape, part.dtype) for part in computed),
            in_specs=[in_vmem] * 3,
            out_specs=(in_hbm,) * 3,
            scratch_shapes=[sems(3)],
            compiler_params=pltpu.CompilerParams(vmem_limit_bytes=1024 * 1024),
        )(*computed)
        return (
            recon.transpose(1, 0, 2),
            dec_grad.transpose(0, 2, 1),
            latent_grad.transpose(1, 0, 2),
        )

    in_specs = (
        P("lat", None, "tok"),
        P("lat", None, "tok"),
        P(None, "tok", "lat"),
        P(None, "lat"),
        P(None, "lat", "tok"),
        P(None, "lat"),
    )
    out_specs = (P("lat", None, "tok"), P(None, "lat", "tok"), P("tok", None, "lat"))
    return jax.shard_map(local, mesh=mesh, in_specs=in_specs, out_specs=out_specs, check_vma=False)


def solution(mesh):
    nx = mesh.shape["tok"]
    return build(mesh, (4, mesh.shape["lat"] // 8, nx), CLASSES)
```
